32 devices in a mesh: dp: 8 (over y, x, core), fsdp: 4 (over z).
Axes of the slice: x: 2, y: 2, z: 4, core: 2. Of those that a mesh axis runs over, the one named last changes fastest.
Arguments:
- grads: float32 [32, 96, 128], P(('dp', 'fsdp')), may hold values from -0.6 to 0.6
- last_peak: float32 [96], replicated, may hold values from 0.05 to 0.8
- master: float32 [96, 128], P(('dp', 'fsdp')), may hold values from -6 to 6
- moment1: float32 [96, 128], P(('dp', 'fsdp')), may hold values from -6 to 6
- moment2: float32 [96, 128], P(('dp', 'fsdp')), may hold values from 0.25 to 8
Outputs:
- new_master: float32 [96, 128], P(('dp', 'fsdp'))
- new_moment1: float32 [96, 128], P(('dp', 'fsdp'))
- new_moment2: float32 [96, 128], P(('dp', 'fsdp'))
- weights: bfloat16 [96, 128], replicated
- block_peak: float32 [96], replicated
The draws below stay inside these ranges and needn't reach their ends.
All inputs are finite; a program needn't handle non-finite values.
Results may differ from the reference program's by a relative error of at most 0.0035.
Values may be sent and summed in bfloat16 or wider, within the bound.
No kernel may reach another device: no remote copies, remote signals or barrier semaphores. Data moves between devices by JAX's collectives and lax.ppermute only.
A program may use at most 64 MiB of HBM per device.

```python
import math
import jax
import jax.numpy as jnp
from jax import lax

BLOCK = 128
STEP_COUNT = 10
REPLICAS = 32
BLOCKS = 96


def strengthened(values, stream_key, source, target, parts, factor):
    def block_of(dim):
        return (jnp.arange(values.shape[dim]) // (values.shape[dim] // parts)).reshape((-1,) + (1,) * (values.ndim - 1 - dim))

    first = jax.random.permutation(stream_key, parts)[block_of(target)]
    other_side = (block_of(target) + parts // 2) % parts
    return jnp.where((block_of(source) == first) | (block_of(source) == other_side), factor * values, values)


def level_of(key, extent, split, low, high):
    factor_of, own = 1.0, jax.random.fold_in(key, 6)
    for axis_at, shards_of in split:
        draws = jnp.exp(jax.random.uniform(jax.random.fold_in(own, axis_at), (shards_of,), jnp.float32, low / len(split), high / len(split)))
        factor_of = factor_of * jnp.repeat(draws, extent[axis_at] // shards_of).reshape([-1 if axis == axis_at else 1 for axis in range(len(extent))])
    return factor_of


def scatter_about(own_key, extent, spread, reach, shards=(), kind=jnp.bfloat16):
    drawn = spread * jax.random.normal(own_key, extent, jnp.float32)
    if shards:
        drawn = drawn * level_of(own_key, extent, shards, -0.22, 0.18)
    return jnp.clip(drawn, -reach, reach).astype(kind)


def gaussian_with(own_key, shape, width, most, cuts, heavy, held_as=jnp.bfloat16):
    entries = width * jax.random.normal(own_key, shape, jnp.float32)
    if cuts:
        entries = entries * level_of(own_key, shape, cuts, -0.22, 0.18)
    return jnp.clip(strengthened(entries, jax.random.fold_in(own_key, 3), *heavy), -most, most).astype(held_as)


def setup_inputs(seed: int = 0) -> dict:
    seeds = jax.random.split(jax.random.key(seed), 6)
    return {
        "grads": gaussian_with(seeds[0], (REPLICAS, BLOCKS, BLOCK), 0.1, 0.6, ((0, 32),), (0, 1, 32, 2.75), jnp.float32),
        "last_peak": jnp.clip(jnp.exp(jax.random.uniform(seeds[1], (BLOCKS,), jnp.float32, math.log(0.05), math.log(0.8))), 0.05, 0.8),
        "master": scatter_about(seeds[2], (BLOCKS, BLOCK), 1.0, 6.0, ((0, 32),), jnp.float32),
        "moment1": scatter_about(seeds[3], (BLOCKS, BLOCK), 1.0, 6.0, ((0, 32),), jnp.float32),
        "moment2": jnp.clip(jnp.exp(math.log(8.0) - 3.465736 * jax.random.uniform(seeds[4], (BLOCKS, BLOCK), jnp.float32) ** level_of(seeds[4], (BLOCKS, BLOCK), ((0, 32),), -0.2, 0.2)), 0.25, 8.0),
    }


code_limit = 448.0
peak_floor = 0.05
beta_one = 0.9
beta_two = 0.95
learn_rate = 0.05
decay_rate = 0.1
epsilon = 1e-08

def quantize(rows, inverse):
    codes = jnp.clip(rows * inverse[:, None], -code_limit, code_limit).astype(jnp.bfloat16)
    return lax.optimization_barrier(codes).astype(jnp.float32)

def adamw(gradient, master, moment1, moment2):
    first = beta_one * moment1 + (1.0 - beta_one) * gradient
    second = beta_two * moment2 + (1.0 - beta_two) * gradient * gradient
    corrected_one = first / (1.0 - beta_one ** STEP_COUNT)
    corrected_two = second / (1.0 - beta_two ** STEP_COUNT)
    updated = master - learn_rate * (corrected_one / (jnp.sqrt(corrected_two) + epsilon) + decay_rate * master)
    return (updated, first, second)

def reference(grads, last_peak, master, moment1, moment2):

    def peak_step(carry, slab):
        return (jnp.maximum(carry, lax.optimization_barrier(jnp.max(jnp.abs(slab), axis=1))), None)
    peak, unused = lax.scan(peak_step, jnp.zeros((grads.shape[1],), jnp.float32), grads)
    floored = jnp.maximum(last_peak, peak_floor)
    inverse = code_limit / floored
    scale = floored / code_limit

    def add_step(total, slab):
        return (total + quantize(slab, inverse), None)
    summed, unused = lax.scan(add_step, jnp.zeros(grads.shape[1:], jnp.float32), grads)
    gradient = summed * scale[:, None]
    updated, first, second = adamw(gradient, master, moment1, moment2)
    return (updated, first, second, updated.astype(jnp.bfloat16), peak)
```

```python
import jax
import jax.numpy as jnp
from jax import lax
from jax.sharding import PartitionSpec as P

STEP_COUNT = 10


code_limit = 448.0
peak_floor = 0.05
beta_one = 0.9
beta_two = 0.95
learn_rate = 0.05
decay_rate = 0.1
epsilon = 1e-08

axes = ("dp", "fsdp")


def adamw(gradient, master, moment1, moment2):
    first = beta_one * moment1 + (1.0 - beta_one) * gradient
    second = beta_two * moment2 + (1.0 - beta_two) * gradient * gradient
    corrected_one = first / (1.0 - beta_one**STEP_COUNT)
    corrected_two = second / (1.0 - beta_two**STEP_COUNT)
    updated = master - learn_rate * (
        corrected_one / (jnp.sqrt(corrected_two) + epsilon) + decay_rate * master
    )
    return (updated, first, second)


def pieces_of(values):
    high = lax.reduce_precision(values, 8, 7)
    rest = values - high
    middle = lax.reduce_precision(rest, 8, 7)
    return (high, middle, rest - middle)


def packed_row(values, width):
    flat = jnp.concatenate(pieces_of(values), axis=-1)
    rows = -(-flat.shape[-1] // width)
    pad = [(0, 0)] * (flat.ndim - 1) + [(0, rows * width - flat.shape[-1])]
    return jnp.pad(flat, pad).reshape(*flat.shape[:-1], rows, width).astype(jnp.bfloat16)


def unpacked_row(rows, count):
    flat = rows.reshape(*rows.shape[:-2], -1).astype(jnp.float32)
    return (flat[..., :count] + flat[..., count : 2 * count]) + flat[..., 2 * count : 3 * count]


def body(grads, last_peak, master, moment1, moment2):
    owned, width = master.shape
    devices = grads.shape[1] // owned
    local = grads.reshape(devices, owned, width)
    floored = jnp.maximum(last_peak, peak_floor)
    inverse = (code_limit / floored).reshape(devices, owned, 1)
    scale = floored / code_limit
    codes = jnp.clip(local * inverse, -code_limit, code_limit).astype(jnp.bfloat16)
    local_peak = jnp.max(jnp.abs(local), axis=2)
    sent = jnp.concatenate([codes, packed_row(local_peak, width)], axis=1)
    got = lax.all_to_all(sent, axes, 0, 0, tiled=True)
    summed = jnp.sum(got[:, :owned].astype(jnp.float32), axis=0)
    own_peak = jnp.max(unpacked_row(got[:, owned:], owned), axis=0)
    own_scale = lax.dynamic_slice_in_dim(scale, lax.axis_index(axes) * owned, owned, 0)
    gradient = summed * own_scale[:, None]
    updated, first, second = adamw(gradient, master, moment1, moment2)
    mine = jnp.concatenate([updated.astype(jnp.bfloat16), packed_row(own_peak, width)], axis=0)
    everyone = jnp.broadcast_to(mine[None], (devices, *mine.shape))
    spread = lax.all_to_all(everyone, axes, 0, 0, tiled=True)
    weights = spread[:, :owned].reshape(devices * owned, width)
    peak = unpacked_row(spread[:, owned:], owned).reshape(devices * owned)
    return (updated, first, second, weights, peak)


def solution(mesh):
    rows = P(axes, None)
    return jax.shard_map(
        body,
        mesh=mesh,
        in_specs=(P(axes, None, None), P(), rows, rows, rows),
        out_specs=(rows, rows, rows, P(), P()),
        check_vma=False,
    )
```
